32 devices in a mesh: fsdp: 16 (over z, y, core), grp: 2 (over x).
Axes of the slice: x: 2, y: 2, z: 4, core: 2. Of those that a mesh axis runs over, the one named last changes fastest.
Arguments:
- hidden: bfloat16 [8192, 3072], P('fsdp', 'grp'), may hold values from -16 to 16
- queries: bfloat16 [8192, 1536], P('fsdp', 'grp'), may hold values from -6 to 6
- attn_keys: bfloat16 [8192, 1536], P('fsdp', 'grp'), may hold values from -6 to 6
- w_value: bfloat16 [1536, 3072], P('fsdp', 'grp'), may hold values from -1 to 1
- w_out: bfloat16 [1536, 3072], P('fsdp', 'grp'), may hold values from -1 to 1
- alpha: float32 [3072], P('grp'), may hold values from 0.05 to 0.5
- out_grad: bfloat16 [8192, 3072], P('fsdp', 'grp'), may hold values from -6 to 6
Outputs:
- new_hidden: bfloat16 [8192, 3072], P('fsdp', 'grp')
- grad_hidden: bfloat16 [8192, 3072], P('fsdp', 'grp')
- grad_queries: bfloat16 [8192, 1536], P('fsdp', 'grp')
- grad_keys: bfloat16 [8192, 1536], P('fsdp', 'grp')
- grad_w_value: float32 [1536, 3072], P('fsdp', 'grp')
- grad_w_out: float32 [1536, 3072], P('fsdp', 'grp')
The draws below stay inside these ranges and needn't reach their ends.
All inputs are finite; a program needn't handle non-finite values.
Results may differ from the reference program's by a relative error of at most 0.012.
The reference program's roundings to bfloat16 on the way count: a program that leaves them out, or rounds other values in their place, can miss the bound.
Values may be sent and summed in bfloat16 or wider, within the bound.
A program may use at most 192 MiB of HBM per device.

```python
import math
import jax
import jax.numpy as jnp
from jax import lax

D = 3072
HEADS = 12
HS = 128
SEQ = 512
HD = 1536
TOKENS = 8192


def column_scales(scale_key, width):
    position = jnp.arange(width, dtype=jnp.float32) / (width - 1)
    ramp_scale = jnp.exp(jnp.log(3.0) * (position - 0.5))
    roughness = jnp.exp(jax.random.uniform(scale_key, (width,), jnp.float32, -1.0, 1.0))
    return ramp_scale * roughness


def draw_hidden(key, part):
    row_key, col_key, val_key = jax.random.split(jax.random.fold_in(key, 5), 3)
    row_scale = jnp.exp(jax.random.uniform(row_key, (TOKENS, 1), jnp.float32, -1.15, 1.15))
    col_scale = column_scales(col_key, D)
    base_draw = jax.random.normal(val_key, (TOKENS, D), jnp.float32)
    return jnp.clip(base_draw * row_scale * col_scale, -16.0, 16.0).astype(jnp.bfloat16)


def weight_rows(key):
    row_key, col_key, val_key = jax.random.split(key, 3)
    row_scale = jnp.exp(jax.random.uniform(row_key, (HD, 1), jnp.float32, 0.0, jnp.log(10.0)))
    col_scale = column_scales(col_key, D)
    base_draw = jax.random.normal(val_key, (HD, D), jnp.float32)
    scaled = base_draw * row_scale * col_scale / (10.0 * D ** 0.5)
    return jnp.clip(scaled, -1.0, 1.0).astype(jnp.bfloat16)


def draw_w_value(key, part):
    return weight_rows(jax.random.fold_in(key, 11))


def draw_w_out(key, part):
    return weight_rows(jax.random.fold_in(key, 23))


def attention_pair(key):
    query_key, keys_key = jax.random.split(jax.random.fold_in(key, 37), 2)
    query_draw = jnp.clip(jax.random.normal(query_key, (TOKENS, HD), jnp.float32), -6.0, 6.0)
    keys_draw = jnp.clip(jax.random.normal(keys_key, (TOKENS, HD), jnp.float32), -6.0, 6.0)
    return (query_draw, keys_draw)


def draw_queries(key, part):
    return attention_pair(key)[0].astype(jnp.bfloat16)


def draw_attn_keys(key, part):
    return attention_pair(key)[1].astype(jnp.bfloat16)


def levels(own_key, shape, cuts, low, high):
    def one(dim, blocks):
        draws = jax.random.uniform(jax.random.fold_in(jax.random.fold_in(own_key, 6), dim), (blocks,), jnp.float32, low / len(cuts), high / len(cuts))
        return jnp.repeat(jnp.exp(draws), shape[dim] // blocks).reshape((-1,) + (1,) * (len(shape) - dim - 1))

    gain = one(*cuts[0])
    for cut in cuts[1:]:
        gain = gain * one(*cut)
    return gain


def gaussian(key, shape, scale, limit, shards=(), kind=jnp.bfloat16):
    loudness = levels(key, shape, shards, -0.22, 0.18) if shards else 1.0
    values = jax.random.normal(key, shape, jnp.float32) * scale * loudness
    return jnp.minimum(jnp.maximum(values, -limit), limit).astype(kind)


def setup_inputs(seed: int = 0) -> dict:
    seeds = jax.random.split(jax.random.key(seed), 8)
    hidden = draw_hidden(jax.random.fold_in(seeds[7], 71), 0)
    queries = draw_queries(jax.random.fold_in(seeds[7], 71), 0)
    attn_keys = draw_attn_keys(jax.random.fold_in(seeds[7], 71), 0)
    w_value = draw_w_value(jax.random.fold_in(seeds[7], 71), 0)
    w_out = draw_w_out(jax.random.fold_in(seeds[7], 71), 0)
    alpha = jnp.clip(jnp.exp(math.log(0.5) - 2.3025851 * jax.random.uniform(seeds[5], (D,), jnp.float32) ** levels(seeds[5], (D,), ((0, 2),), -0.2, 0.2)), 0.05, 0.5)
    out_grad = gaussian(seeds[6], (TOKENS, D), 1.0, 6.0, ((0, 16), (1, 2)))
    return dict(hidden=hidden, queries=queries, attn_keys=attn_keys, w_value=w_value, w_out=w_out, alpha=alpha, out_grad=out_grad)


EPS = 1e-06

def contract_last(left, right):
    return lax.dot_general(left, right, (((1,), (1,)), ((), ())), preferred_element_type=jnp.float32)

def contract_first(left, right):
    return lax.dot_general(left, right, (((0,), (0,)), ((), ())), preferred_element_type=jnp.float32)

def causal_probs(query_head, key_head):
    length = query_head.shape[0]
    score_scale = query_head.shape[1] ** (-0.5)
    scores = contract_last(query_head, key_head) * score_scale
    row_pos = lax.broadcasted_iota(jnp.int32, (length, length), 0)
    col_pos = lax.broadcasted_iota(jnp.int32, (length, length), 1)
    scores = jnp.where(row_pos >= col_pos, scores, -1e+30)
    row_peak = lax.optimization_barrier(jnp.max(scores, axis=1, keepdims=True))
    exp_terms = jnp.exp(scores - row_peak)
    return exp_terms / lax.optimization_barrier(jnp.sum(exp_terms, axis=1, keepdims=True))

def head_forward(items):
    query_head, key_head, value_head = items
    attn_prob = causal_probs(query_head, key_head)
    return jnp.dot(attn_prob.astype(jnp.bfloat16), value_head, preferred_element_type=jnp.float32).astype(jnp.bfloat16)

def head_backward(items):
    query_head, key_head, value_head, grad_head = items
    score_scale = query_head.shape[1] ** (-0.5)
    attn_prob = causal_probs(query_head, key_head)
    prob_half = attn_prob.astype(jnp.bfloat16)
    grad_prob = contract_last(grad_head, value_head)
    row_delta = lax.optimization_barrier(jnp.sum(attn_prob * grad_prob, axis=1, keepdims=True))
    grad_score = (attn_prob * (grad_prob - row_delta)).astype(jnp.bfloat16)
    grad_query = (jnp.dot(grad_score, key_head, preferred_element_type=jnp.float32) * score_scale).astype(jnp.bfloat16)
    grad_key = (contract_first(grad_score, query_head) * score_scale).astype(jnp.bfloat16)
    grad_value = contract_first(prob_half, grad_head).astype(jnp.bfloat16)
    return (grad_query, grad_key, grad_value)

def to_heads(block):
    return block.reshape(TOKENS // SEQ, SEQ, HEADS, HS).transpose(0, 2, 1, 3).reshape(-1, SEQ, HS)

def from_heads(stacked):
    return stacked.reshape(TOKENS // SEQ, HEADS, SEQ, HS).transpose(0, 2, 1, 3).reshape(TOKENS, HEADS * HS)

def unit_rows(weights):
    weights_f = weights.astype(jnp.float32)
    norms = jnp.sqrt(lax.optimization_barrier(jnp.sum(weights_f * weights_f, axis=1, keepdims=True)) + EPS)
    return (weights_f / norms, norms)

def unit_back(grad_unit, unit, norms):
    row_dot = lax.optimization_barrier(jnp.sum(grad_unit * unit, axis=1, keepdims=True))
    return (grad_unit - unit * row_dot) / norms

def reference(hidden, queries, attn_keys, w_value, w_out, alpha, out_grad):
    unit_v, norm_v = unit_rows(w_value)
    unit_o, norm_o = unit_rows(w_out)
    weight_v = unit_v.astype(jnp.bfloat16)
    weight_o = unit_o.astype(jnp.bfloat16)
    values = contract_last(hidden, weight_v).astype(jnp.bfloat16)
    q_heads = to_heads(queries)
    k_heads = to_heads(attn_keys)
    v_heads = to_heads(values)
    attn = from_heads(lax.map(head_forward, (q_heads, k_heads, v_heads)))
    proj = jnp.dot(attn, weight_o, preferred_element_type=jnp.float32)
    hidden_f = hidden.astype(jnp.float32)
    proj_rs = lax.rsqrt(lax.optimization_barrier(jnp.mean(proj * proj, axis=1, keepdims=True)) + EPS)
    mixed = hidden_f + alpha * (proj * proj_rs - hidden_f)
    mix_rs = lax.rsqrt(lax.optimization_barrier(jnp.mean(mixed * mixed, axis=1, keepdims=True)) + EPS)
    new_hidden = (mixed * mix_rs).astype(jnp.bfloat16)
    grad_out = out_grad.astype(jnp.float32)
    grad_mix = mix_rs * (grad_out - mixed * mix_rs * mix_rs * lax.optimization_barrier(jnp.mean(grad_out * mixed, axis=1, keepdims=True)))
    grad_res = grad_mix * (1.0 - alpha)
    grad_pn = grad_mix * alpha
    grad_proj = proj_rs * (grad_pn - proj * proj_rs * proj_rs * lax.optimization_barrier(jnp.mean(grad_pn * proj, axis=1, keepdims=True)))
    grad_proj_b = grad_proj.astype(jnp.bfloat16)
    grad_attn = contract_last(grad_proj_b, weight_o).astype(jnp.bfloat16)
    gw_o = contract_first(attn, grad_proj_b)
    grad_q, grad_k, grad_v = lax.map(head_backward, (q_heads, k_heads, v_heads, to_heads(grad_attn)))
    grad_values = from_heads(grad_v)
    grad_hidden = (grad_res + jnp.dot(grad_values, weight_v, preferred_element_type=jnp.float32)).astype(jnp.bfloat16)
    gw_v = contract_first(grad_values, hidden)
    grad_w_value = unit_back(gw_v, unit_v, norm_v)
    grad_w_out = unit_back(gw_o, unit_o, norm_o)
    return (new_hidden, grad_hidden, from_heads(grad_q), from_heads(grad_k), grad_w_value, grad_w_out)
```

```python
import jax
import jax.numpy as jnp
from jax import lax
from jax.experimental import pallas as pl
from jax.experimental.pallas import tpu as pltpu
from jax.sharding import PartitionSpec as P

D = 3072
HS = 128


EPS = 1e-06


def contract_last(left, right):
    return lax.dot_general(
        left, right, (((1,), (1,)), ((), ())), preferred_element_type=jnp.float32
    )


def contract_first(left, right):
    return lax.dot_general(
        left, right, (((0,), (0,)), ((), ())), preferred_element_type=jnp.float32
    )


def cost(flops, nbytes):
    return pl.CostEstimate(flops=flops, bytes_accessed=nbytes, transcendentals=0)


def probs_kernel(q_ref, k_ref, probs_ref):
    length = q_ref.shape[0]
    score_scale = q_ref.shape[1] ** (-0.5)
    scores = contract_last(q_ref[...], k_ref[...]) * score_scale
    row_pos = lax.broadcasted_iota(jnp.int32, (length, length), 0)
    col_pos = lax.broadcasted_iota(jnp.int32, (length, length), 1)
    scores = jnp.where(row_pos >= col_pos, scores, -1e30)
    row_peak = jnp.max(scores, axis=1, keepdims=True)
    exp_terms = jnp.exp(scores - row_peak)
    probs_ref[0] = exp_terms * (1.0 / jnp.sum(exp_terms, axis=1, keepdims=True))


def forward_kernel(probs_ref, part_ref, recv_ref, scale_ref, attn_ref, values_ref):
    values = (part_ref[...] + recv_ref[...].astype(jnp.float32)) * scale_ref[...]
    values_b = values.astype(jnp.bfloat16)
    values_ref[...] = values_b
    attn_ref[...] = jnp.dot(
        probs_ref[0].astype(jnp.bfloat16), values_b, preferred_element_type=jnp.float32
    ).astype(jnp.bfloat16)


def backward_kernel(
    probs_ref, q_ref, k_ref, v_ref, part_ref, recv_ref, gq_ref, gk_ref, gv_ref
):
    score_scale = q_ref.shape[1] ** (-0.5)
    grad_head = (part_ref[...] + recv_ref[...].astype(jnp.float32)).astype(jnp.bfloat16)
    probs = probs_ref[0]
    grad_prob = contract_last(grad_head, v_ref[...])
    row_delta = jnp.sum(probs * grad_prob, axis=1, keepdims=True)
    grad_score = (probs * (grad_prob - row_delta)).astype(jnp.bfloat16)
    gv_ref[...] = contract_first(probs.astype(jnp.bfloat16), grad_head).astype(jnp.bfloat16)
    gq_ref[...] = (
        jnp.dot(grad_score, k_ref[...], preferred_element_type=jnp.float32) * score_scale
    ).astype(jnp.bfloat16)
    gk_ref[...] = (contract_first(grad_score, q_ref[...]) * score_scale).astype(jnp.bfloat16)


def head_spec(length):
    return pl.BlockSpec((length, HS), lambda h: (0, h))


def square_spec(length):
    return pl.BlockSpec((1, length, length), lambda h: (h, 0, 0))


def head_probs(queries, keys):
    length, width = queries.shape
    heads = width // HS
    return pl.pallas_call(
        probs_kernel,
        grid=(heads,),
        in_specs=[head_spec(length)] * 2,
        out_specs=square_spec(length),
        out_shape=jax.ShapeDtypeStruct((heads, length, length), jnp.float32),
        cost_estimate=cost(heads * 30 * HS * length * length, 4 * heads * length * length),
    )(queries, keys)


def attend(probs, part, recv, scale):
    length, width = part.shape
    heads = width // HS
    one = head_spec(length)
    shape = jax.ShapeDtypeStruct((length, width), jnp.bfloat16)
    return pl.pallas_call(
        forward_kernel,
        grid=(heads,),
        in_specs=[square_spec(length), one, one, pl.BlockSpec((1, HS), lambda h: (0, h))],
        out_specs=[one, one],
        out_shape=[shape, shape],
        cost_estimate=cost(heads * 4 * HS * length * length, 6 * heads * length * length),
    )(probs, part, recv, scale)


def attend_backward(probs, queries, keys, values, part, recv):
    length, width = part.shape
    heads = width // HS
    one = head_spec(length)
    shape = jax.ShapeDtypeStruct((length, width), jnp.bfloat16)
    return pl.pallas_call(
        backward_kernel,
        grid=(heads,),
        in_specs=[square_spec(length)] + [one] * 5,
        out_specs=[one] * 3,
        out_shape=[shape] * 3,
        cost_estimate=cost(heads * 30 * HS * length * length, 6 * heads * length * length),
    )(probs, queries, keys, values, part, recv)


def shards(hidden, queries, attn_keys, w_value, w_out, alpha, out_grad):
    groups = lax.axis_size("grp")
    assert groups == 2
    me = lax.axis_index("grp")
    swap = [(0, 1), (1, 0)]

    def exchange(block):
        return lax.ppermute(block, "grp", swap)

    def mine_and_other(weight):
        rows = weight.shape[0] // groups
        return (
            lax.dynamic_slice_in_dim(weight, me * rows, rows, 0),
            lax.dynamic_slice_in_dim(weight, (1 - me) * rows, rows, 0),
        )

    def in_order(mine, other):
        return jnp.concatenate(
            (jnp.where(me == 0, mine, other), jnp.where(me == 0, other, mine)), axis=1
        )

    raw_v = lax.all_gather(w_value, "fsdp", axis=0, tiled=True)
    value_rows = w_value.astype(jnp.float32)
    out_rows = w_out.astype(jnp.float32)
    own_sums = jnp.stack(
        (jnp.sum(value_rows * value_rows, axis=1), jnp.sum(out_rows * out_rows, axis=1))
    )
    own_sums = own_sums + exchange(own_sums)
    norms = jnp.sqrt(own_sums + EPS)
    norm_v = norms[0][:, None]
    norm_o = norms[1][:, None]
    unit_v = value_rows / norm_v
    unit_o = out_rows / norm_o
    weight_o = lax.all_gather(unit_o.astype(jnp.bfloat16), "fsdp", axis=0, tiled=True)
    probs = head_probs(queries, attn_keys)

    raw_mine, raw_other = mine_and_other(raw_v)
    value_recv = exchange(contract_last(hidden, raw_other).astype(jnp.bfloat16))
    value_part = contract_last(hidden, raw_mine)
    raw_rows = raw_v.astype(jnp.float32)
    raw_sums = jnp.sum(raw_rows * raw_rows, axis=1)
    all_norm_v = jnp.sqrt(raw_sums + exchange(raw_sums) + EPS)
    width = queries.shape[1]
    scale = 1.0 / lax.dynamic_slice_in_dim(all_norm_v, me * width, width, 0)
    attn_mine, values = attend(probs, value_part, value_recv, scale[None, :])
    weight_v = (raw_v.astype(jnp.float32) / all_norm_v[:, None]).astype(jnp.bfloat16)
    attn_all = in_order(attn_mine, exchange(attn_mine))
    proj = jnp.dot(attn_all, weight_o, preferred_element_type=jnp.float32)
    hidden_f = hidden.astype(jnp.float32)
    keep_rate = 1.0 - alpha
    grad_out = out_grad.astype(jnp.float32)
    moments = jnp.stack(
        (
            jnp.sum(proj * proj, axis=1),
            jnp.sum(keep_rate * keep_rate * hidden_f * hidden_f, axis=1),
            jnp.sum(keep_rate * alpha * hidden_f * proj, axis=1),
            jnp.sum(alpha * alpha * proj * proj, axis=1),
            jnp.sum(grad_out * keep_rate * hidden_f, axis=1),
            jnp.sum(grad_out * alpha * proj, axis=1),
        )
    )
    moments = moments + exchange(moments)
    proj_rs = lax.rsqrt(moments[0] / D + EPS)[:, None]
    cross_sum = moments[2][:, None]
    alpha_sum = moments[3][:, None]
    mix_mean = (moments[1][:, None] + 2.0 * proj_rs * cross_sum + proj_rs * proj_rs * alpha_sum) / D
    mix_rs = lax.rsqrt(mix_mean + EPS)
    mixed = hidden_f + alpha * (proj * proj_rs - hidden_f)
    new_hidden = (mixed * mix_rs).astype(jnp.bfloat16)
    grad_mean = (moments[4][:, None] + proj_rs * moments[5][:, None]) / D
    grad_mix = mix_rs * (grad_out - mixed * mix_rs * mix_rs * grad_mean)
    grad_pn = grad_mix * alpha
    proj_mean = (
        mix_rs * moments[5][:, None]
        - mix_rs * mix_rs * mix_rs * grad_mean * (cross_sum + proj_rs * alpha_sum)
    ) / D
    grad_res = grad_mix * keep_rate
    grad_proj = proj_rs * (grad_pn - proj * proj_rs * proj_rs * proj_mean)
    grad_proj_b = grad_proj.astype(jnp.bfloat16)
    out_mine, out_other = mine_and_other(weight_o)
    grad_recv = exchange(contract_last(grad_proj_b, out_other).astype(jnp.bfloat16))
    grad_part = contract_last(grad_proj_b, out_mine)
    gw_o_own = lax.psum_scatter(
        contract_first(attn_all, grad_proj_b).astype(jnp.bfloat16),
        "fsdp",
        scatter_dimension=0,
        tiled=True,
    ).astype(jnp.float32)
    grad_q, grad_k, grad_v = attend_backward(
        probs, queries, attn_keys, values, grad_part, grad_recv
    )
    grad_values = in_order(grad_v, exchange(grad_v))
    gw_v_own = lax.psum_scatter(
        contract_first(grad_values, hidden).astype(jnp.bfloat16),
        "fsdp",
        scatter_dimension=0,
        tiled=True,
    ).astype(jnp.float32)
    grad_hidden = (
        grad_res + jnp.dot(grad_values, weight_v, preferred_element_type=jnp.float32)
    ).astype(jnp.bfloat16)
    dot_o = jnp.sum(gw_o_own * unit_o, axis=1, keepdims=True)
    dot_o = dot_o + exchange(dot_o)
    grad_w_out = (gw_o_own - unit_o * dot_o) / norm_o
    dot_v = jnp.sum(gw_v_own * unit_v, axis=1, keepdims=True)
    dot_v = dot_v + exchange(dot_v)
    grad_w_value = (gw_v_own - unit_v * dot_v) / norm_v
    return (new_hidden, grad_hidden, grad_q, grad_k, grad_w_value, grad_w_out)


MESH = pl.DeviceIdType.MESH
BLOCK = 256
BF = jnp.bfloat16
F32 = jnp.float32


def nearest(z, s, count):
    reach = jnp.minimum(z, count - 1 - z)
    both = z - (s + 1) // 2 if s % 2 else z + s // 2
    rest = jnp.where(z <= count - 1 - z, s, count - 1 - s)
    return jnp.where(s <= 2 * reach, both, rest)


def layer_kernel(
    hid, q, k, wv, wo, alpha, og,
    nh, gh, gq, gk, gwv, gwo,
    all_v, all_o, probs, nrm, part, xsend, xrecv, vals, attn, proj, gpb, mom, momx, gval,
    grad_s, big_o, ra, rb, rc, acc, fin, dots,
    z_in, z_out, y_in, y_out, c_in, c_out,
    a_in, a_out, b_in, b_out, r_in, r_out, x_in, x_out, s_in, s_out,
):
    tokens, width = hid.shape
    rows = wv.shape[0]
    heads = part.shape[0]
    devices = all_v.shape[0] // rows
    line = devices // 4
    unit = 4 * rows
    per_unit = unit // HS
    own_units = line // 2
    score_scale = HS ** (-0.5)
    full = 2 * width

    me = lax.axis_index("fsdp")
    g = lax.axis_index("grp")
    z = me // 4
    y = lax.rem(me // 2, 2)
    c = lax.rem(me, 2)
    right, left = me + 4, me - 4
    across = z * 4 + (1 - y) * 2 + c
    sibling = z * 4 + y * 2 + (1 - c)
    low = g * own_units
    other_low = (1 - g) * own_units

    def copy(src, dst, out_sem, in_sem, dev):
        return pltpu.make_async_remote_copy(
            src_ref=src, dst_ref=dst, send_sem=out_sem, recv_sem=in_sem,
            device_id=dev, device_id_type=MESH,
        )

    def xcopy(src, dst, kind, h):
        return copy(src, dst, x_out.at[kind, h], x_in.at[kind, h], {"grp": 1 - g})

    def scopy(src, dst, i):
        return copy(src, dst, s_out.at[i], s_in.at[i], {"grp": 1 - g})

    barrier = pltpu.get_barrier_semaphore()

    def greet(dev):
        pl.semaphore_signal(barrier, inc=1, device_id=dev, device_id_type=MESH)

    greet({"grp": 1 - g})
    greet({"fsdp": across})
    greet({"fsdp": sibling})
    pl.when(z > 0)(lambda: greet({"fsdp": left}))
    pl.when(z < line - 1)(lambda: greet({"fsdp": right}))

    lane = lax.broadcasted_iota(jnp.int32, (rows, HS), 1)

    def row_sums(first, second):
        return jnp.where(
            lane == 0,
            jnp.sum(first, axis=1, keepdims=True),
            jnp.sum(second, axis=1, keepdims=True),
        )

    wv_f = wv[...].astype(F32)
    wo_f = wo[...].astype(F32)
    nrm[0] = row_sums(wv_f * wv_f, wo_f * wo_f)
    pl.semaphore_wait(
        barrier, 3 + (z > 0).astype(jnp.int32) + (z < line - 1).astype(jnp.int32)
    )
    norm_copy = scopy(nrm.at[0], nrm.at[1], 0)
    norm_copy.start()

    def cols(h):
        return pl.ds(pl.multiple_of(h * HS, HS), HS)

    def probs_head(h):
        qh = q[:, cols(h)]
        kh = k[:, cols(h)]
        for r in range(tokens // BLOCK):
            top, reach = r * BLOCK, (r + 1) * BLOCK
            scores = contract_last(qh[top:reach], kh[:reach]) * score_scale
            row_pos = lax.broadcasted_iota(jnp.int32, (BLOCK, reach), 0) + top
            col_pos = lax.broadcasted_iota(jnp.int32, (BLOCK, reach), 1)
            scores = jnp.where(row_pos >= col_pos, scores, -1e30)
            terms = jnp.exp(scores - jnp.max(scores, axis=1, keepdims=True))
            total = jnp.sum(terms, axis=1, keepdims=True)
            probs[h, top:reach, :reach] = (terms * (1.0 / total)).astype(BF)

    probs_head(0)
    norm_copy.wait()
    inv = lax.rsqrt(nrm[0] + nrm[1] + EPS)

    def my_rows(ref):
        return ref.at[pl.ds(pl.multiple_of(me * rows, rows), rows)]

    my_rows(all_v)[...] = (wv[...].astype(F32) * inv[:, 0:1]).astype(BF)
    my_rows(all_o)[...] = (wo[...].astype(F32) * inv[:, 1:2]).astype(BF)

    def shard(ref, u, yy, cc):
        start = pl.multiple_of((u * 4 + yy * 2 + cc) * rows, rows)
        return ref.at[pl.ds(start, rows)]

    def unit_rows(ref, u):
        return ref.at[pl.ds(pl.multiple_of(u * unit, unit), unit)]

    gathered = (all_v, all_o)

    def go_line(w, u, way, dev):
        block = shard(gathered[w], u, y, c)
        return copy(block, block, z_out.at[w, u, way], z_in.at[w, u], {"fsdp": dev})

    def go_across(w, u):
        block = shard(gathered[w], u, y, c)
        return copy(block, block, y_out.at[w, u], y_in.at[w, u], {"fsdp": across})

    def from_across(w, u):
        block = shard(gathered[w], u, 1 - y, c)
        return copy(block, block, y_out.at[w, u], y_in.at[w, u], {"fsdp": across})

    def go_sibling(w, u, yy):
        block = shard(gathered[w], u, yy, c)
        return copy(block, block, c_out.at[w, u, yy], c_in.at[w, u, yy], {"fsdp": sibling})

    def from_sibling(w, u, yy):
        block = shard(gathered[w], u, yy, 1 - c)
        return copy(block, block, c_out.at[w, u, yy], c_in.at[w, u, yy], {"fsdp": sibling})

    def on_line(w, u, act):
        pl.when((u <= z) & (z < line - 1))(lambda: act(go_line(w, u, 1, right)))
        pl.when((u >= z) & (z > 0))(lambda: act(go_line(w, u, 0, left)))

    def gather_step(w, s):
        u = nearest(z, s, line)
        if s:
            go_line(w, u, 0, left).wait_recv()
        on_line(w, u, lambda d: d.start())
        go_across(w, u).start()
        go_sibling(w, u, y).start()

    def gather_across(w, s):
        u = nearest(z, s, line)
        from_across(w, u).wait_recv()
        go_sibling(w, u, 1 - y).start()

    def gather_sibling(w, s):
        u = nearest(z, s, line)
        from_sibling(w, u, 0).wait_recv()
        from_sibling(w, u, 1).wait_recv()

    def gather_drain(w):
        def one(u, carry):
            on_line(w, u, lambda d: d.wait_send())
            go_across(w, u).wait_send()
            go_sibling(w, u, 0).wait_send()
            go_sibling(w, u, 1).wait_send()
            return carry

        lax.fori_loop(0, line, one, 0)

    def is_own(u):
        return (u >= low) & (u < low + own_units)

    def split_heads(kind, u, block):
        @pl.when(is_own(u))
        def _():
            for j in range(per_unit):
                part[(u - low) * per_unit + j] = block[:, j * HS : (j + 1) * HS]

        @pl.when(jnp.logical_not(is_own(u)))
        def _():
            for j in range(per_unit):
                h = (u - other_low) * per_unit + j
                xsend[kind, h] = block[:, j * HS : (j + 1) * HS].astype(BF)
                xcopy(xsend.at[kind, h], xrecv.at[kind, h], 2 * kind, h).start()

    def value_unit(s):
        u = nearest(z, s, line)
        split_heads(0, u, contract_last(hid[...], unit_rows(all_v, u)[...]))

    gather_step(0, 0)
    todo = list(range(1, heads))
    for s in range(1, line):
        while todo and len(todo) > heads - 1 - 2 * s:
            probs_head(todo.pop(0))
        gather_step(0, s)
        gather_across(0, s - 1)
        gather_sibling(0, s - 1)
        value_unit(s - 1)
    for h in todo:
        probs_head(h)
    gather_step(1, 0)
    gather_across(0, line - 1)
    gather_sibling(0, line - 1)
    value_unit(line - 1)

    def attend_head(h):
        xcopy(xsend.at[0, h], xrecv.at[0, h], 0, h).wait_recv()
        vals[h] = (part[h] + xrecv[0, h].astype(F32)).astype(BF)
        mine = g * heads + h
        for r in range(tokens // BLOCK):
            top, reach = r * BLOCK, (r + 1) * BLOCK
            attn[mine, top:reach] = jnp.dot(
                probs[h, top:reach, :reach], vals[h, :reach], preferred_element_type=F32
            ).astype(BF)
        xcopy(attn.at[mine], attn.at[mine], 1, h).start()

    def own_near(n):
        zc = jnp.clip(z, low, low + own_units - 1) - low
        return nearest(zc, n, own_units)

    for n in range(own_units):
        u = own_near(n)
        lax.fori_loop(0, per_unit, lambda j, x: (attend_head(u * per_unit + j), x)[1], 0)
        gather_step(1, 1 + n)
        gather_across(1, n)

    def heads_of(ref, u):
        return jnp.concatenate([ref[u * per_unit + j] for j in range(per_unit)], axis=1)

    def accumulate(ref, u, weight, fresh):
        add = jnp.dot(heads_of(ref, u), unit_rows(weight, u)[...], preferred_element_type=F32)
        if fresh:
            proj[...] = add
        else:
            proj[...] += add

    def project(s):
        u = nearest(z, s, line)
        gather_sibling(1, s)

        @pl.when(jnp.logical_not(is_own(u)))
        def _():
            for j in range(per_unit):
                h = (u - other_low) * per_unit + j
                there = attn.at[(1 - g) * heads + h]
                xcopy(there, there, 1, h).wait_recv()

        accumulate(attn, u, all_o, s == 0)

    for s in range(line):
        if s + 1 > own_units and s + 1 < line:
            gather_step(1, s + 1)
        if s >= own_units:
            gather_across(1, s)
        project(s)

    rates = alpha[...]
    keep = 1.0 - rates
    step = 16

    def chunk(i):
        return pl.ds(pl.multiple_of(i * step, step), step)

    lane16 = lax.broadcasted_iota(jnp.int32, (step, HS), 1)

    def moments(i, carry):
        r = chunk(i)
        p = proj[r]
        kh = keep * hid[r].astype(F32)
        ap = rates * p
        go = og[r].astype(F32)
        sums = (p * p, kh * kh, kh * ap, ap * ap, go * kh, go * ap)
        out = jnp.zeros((step, HS), F32)
        for n, term in enumerate(sums):
            out = jnp.where(lane16 == n, jnp.sum(term, axis=1, keepdims=True), out)
        mom[r] = out
        return carry

    lax.fori_loop(0, tokens // step, moments, 0)
    for i in range(tokens // HS):
        span = slice(i * HS, (i + 1) * HS)
        momx[0, :, span] = jnp.transpose(mom[span])[:8]
    mom_copy = scopy(momx.at[0], momx.at[1], 1)
    mom_copy.start()
    gather_drain(0)
    gather_drain(1)
    mom_copy.wait()
    for i in range(tokens // HS):
        span = slice(i * HS, (i + 1) * HS)
        total = momx[0, :, span] + momx[1, :, span]
        padded = jnp.concatenate([total, jnp.zeros((HS - 8, HS), F32)], axis=0)
        mom[span] = jnp.transpose(padded)

    def mix(i, carry):
        r = chunk(i)
        m = mom[r]
        s_pp, s_hh, s_hp, s_ap, s_gh, s_gp = [m[:, n : n + 1] for n in range(6)]
        proj_rs = lax.rsqrt(s_pp / full + EPS)
        mix_mean = (s_hh + 2.0 * proj_rs * s_hp + proj_rs * proj_rs * s_ap) / full
        mix_rs = lax.rsqrt(mix_mean + EPS)
        grad_mean = (s_gh + proj_rs * s_gp) / full
        proj_mean = (
            mix_rs * s_gp - mix_rs * mix_rs * mix_rs * grad_mean * (s_hp + proj_rs * s_ap)
        ) / full
        p = proj[r]
        pn = p * proj_rs
        h = hid[r].astype(F32)
        mixed = h + rates * (pn - h)
        normed = mixed * mix_rs
        nh[r] = normed.astype(BF)
        grad_mix = mix_rs * (og[r].astype(F32) - normed * (mix_rs * grad_mean))
        proj[r] = grad_mix * keep
        gpb[r] = (proj_rs * (grad_mix * rates - pn * (proj_rs * proj_mean))).astype(BF)
        return carry

    lax.fori_loop(0, tokens // step, mix, 0)

    def own_back(n):
        return jnp.where(g == 0, n, line - 1 - n)

    def other_back(n):
        return jnp.where(g == 0, line - 1 - n, n)

    for n in range(own_units):
        u = other_back(n)
        split_heads(1, u, contract_last(gpb[...], unit_rows(all_o, u)[...]))
    for n in range(own_units):
        u = own_back(n)
        split_heads(1, u, contract_last(gpb[...], unit_rows(all_o, u)[...]))

    big = (big_o, all_o)

    def weight_grad(w, ref, other, u):
        add = contract_first(heads_of(ref, u), other[...])
        unit_rows(big[w], u)[...] = add.astype(BF)

    def to_sibling(w, u, yy):
        return copy(
            shard(big[w], u, yy, 1 - c), ra.at[w, u, yy],
            a_out.at[w, u, yy], a_in.at[w, u, yy], {"fsdp": sibling},
        )

    def to_across(w, u):
        return copy(
            ra.at[w, u, 1 - y], rb.at[w, u], b_out.at[w, u], b_in.at[w, u], {"fsdp": across}
        )

    def to_line(w, u, way, dev):
        return copy(
            ra.at[w, u, y], rc.at[w, u, 1 - way],
            r_out.at[w, u, way], r_in.at[w, u, 1 - way], {"fsdp": dev},
        )

    def scatter_sibling(w, u):
        to_sibling(w, u, 0).start()
        to_sibling(w, u, 1).start()

    def scatter_across(w, u):
        to_sibling(w, u, 0).wait_recv()
        to_sibling(w, u, 1).wait_recv()
        ra[w, u, 1 - y] = (
            ra[w, u, 1 - y].astype(F32) + shard(big[w], u, 1 - y, c)[...].astype(F32)
        ).astype(BF)
        to_across(w, u).start()

    def scatter_line(w, u):
        to_across(w, u).wait_recv()
        acc[...] = (
            shard(big[w], u, y, c)[...].astype(F32)
            + ra[w, u, y].astype(F32)
            + rb[w, u].astype(F32)
        )

        @pl.when((z > 0) & (u >= z))
        def _():
            to_line(w, u, 1, right).wait_recv()
            acc[...] += rc[w, u, 0].astype(F32)

        @pl.when((z < line - 1) & (u <= z))
        def _():
            to_line(w, u, 0, left).wait_recv()
            acc[...] += rc[w, u, 1].astype(F32)

        @pl.when(u == z)
        def _():
            fin[w] = acc[...]

        @pl.when(u != z)
        def _():
            ra[w, u, y] = acc[...].astype(BF)

        pl.when(u > z)(lambda: to_line(w, u, 1, right).start())
        pl.when(u < z)(lambda: to_line(w, u, 0, left).start())

    def scatter_drain(w):
        def one(u, carry):
            to_sibling(w, u, 0).wait_send()
            to_sibling(w, u, 1).wait_send()
            to_across(w, u).wait_send()
            pl.when(u > z)(lambda: to_line(w, u, 1, right).wait_send())
            pl.when(u < z)(lambda: to_line(w, u, 0, left).wait_send())
            return carry

        lax.fori_loop(0, line, one, 0)

    far_first = [line - 1 - s for s in range(line)]
    for s in far_first:
        u = nearest(z, s, line)
        weight_grad(0, attn, gpb, u)
        scatter_sibling(0, u)

    def back_head(h):
        xcopy(xsend.at[1, h], xrecv.at[1, h], 2, h).wait_recv()
        mine = g * heads + h
        grad_head = (part[h] + xrecv[1, h].astype(F32)).astype(BF)
        qh = q[:, cols(h)]
        kh = k[:, cols(h)]
        vh = vals[h]
        for r in range(tokens // BLOCK):
            top, reach = r * BLOCK, (r + 1) * BLOCK
            p = probs[h, top:reach, :reach].astype(F32)
            grad_prob = contract_last(grad_head[top:reach], vh[:reach])
            delta = jnp.sum(p * grad_prob, axis=1, keepdims=True)
            grad_score = (p * (grad_prob - delta)).astype(BF)
            grad_s[top:reach, :reach] = grad_score
            gq[top:reach, cols(h)] = (
                jnp.dot(grad_score, kh[:reach], preferred_element_type=F32) * score_scale
            ).astype(BF)
        for r in range(tokens // BLOCK):
            top, reach = r * BLOCK, (r + 1) * BLOCK
            gval[mine, top:reach] = contract_first(
                probs[h, top:, top:reach], grad_head[top:]
            ).astype(BF)
            gk[top:reach, cols(h)] = (
                contract_first(grad_s[top:, top:reach], qh[top:]) * score_scale
            ).astype(BF)
        xcopy(gval.at[mine], gval.at[mine], 3, h).start()

    for n in range(own_units):
        u = own_back(n)
        lax.fori_loop(
            0, per_unit, lambda j, x: (back_head((u - low) * per_unit + j), x)[1], 0
        )
        if n == 0:
            for s in far_first:
                scatter_across(0, nearest(z, s, line))
        weight_grad(1, gval, hid, u)
        scatter_sibling(1, u)
        if n < line:
            scatter_line(0, nearest(z, far_first[n], line))
    for n in range(own_units):
        u = own_back(n)
        scatter_across(1, u)
        accumulate(gval, u, all_v, False)
        if own_units + n < line:
            scatter_line(0, nearest(z, far_first[own_units + n], line))

    for n in range(own_units):
        u = other_back(n)
        for j in range(per_unit):
            h = (u - other_low) * per_unit + j
            there = gval.at[(1 - g) * heads + h]
            xcopy(there, there, 3, h).wait_recv()
        weight_grad(1, gval, hid, u)
        scatter_sibling(1, u)
        scatter_line(1, own_back(n))
        scatter_across(1, u)
        accumulate(gval, u, all_v, False)
    gh[...] = proj[...].astype(BF)

    inv = lax.rsqrt(nrm[0] + nrm[1] + EPS)
    unit_v = wv[...].astype(F32) * inv[:, 0:1]
    unit_o = wo[...].astype(F32) * inv[:, 1:2]
    for n in range(own_units):
        scatter_line(1, other_back(n))
    dots[0] = row_sums(fin[1] * unit_v, fin[0] * unit_o)
    dot_copy = scopy(dots.at[0], dots.at[1], 2)
    dot_copy.start()
    scatter_drain(0)
    scatter_drain(1)

    def drain(h, carry):
        xcopy(xsend.at[0, h], xrecv.at[0, h], 0, h).wait_send()
        xcopy(xsend.at[1, h], xrecv.at[1, h], 2, h).wait_send()
        mine = g * heads + h
        xcopy(attn.at[mine], attn.at[mine], 1, h).wait_send()
        xcopy(gval.at[mine], gval.at[mine], 3, h).wait_send()
        return carry

    lax.fori_loop(0, heads, drain, 0)
    dot_copy.wait()
    total = dots[0] + dots[1]
    gwv[...] = (fin[1] - unit_v * total[:, 0:1]) * inv[:, 0:1]
    gwo[...] = (fin[0] - unit_o * total[:, 1:2]) * inv[:, 1:2]


def layer(hidden, queries, attn_keys, w_value, w_out, alpha, out_grad):
    tokens, width = hidden.shape
    rows = w_value.shape[0]
    own = queries.shape[1]
    heads = own // HS
    devices = lax.axis_size("fsdp")
    line = devices // 4
    head_block = (heads, tokens, HS)
    dma = pltpu.SemaphoreType.DMA
    shape = jax.ShapeDtypeStruct
    scratch = [
        pltpu.VMEM((devices * rows, width), BF),
        pltpu.VMEM((devices * rows, width), BF),
        pltpu.VMEM((heads, tokens, tokens), BF),
        pltpu.VMEM((2, rows, HS), F32),
        pltpu.VMEM(head_block, F32),
        pltpu.VMEM((2,) + head_block, BF),
        pltpu.VMEM((2,) + head_block, BF),
        pltpu.VMEM(head_block, BF),
        pltpu.VMEM((2 * heads, tokens, HS), BF),
        pltpu.VMEM((tokens, width), F32),
        pltpu.VMEM((tokens, width), BF),
        pltpu.VMEM((tokens, HS), F32),
        pltpu.VMEM((2, 8, tokens), F32),
        pltpu.VMEM((2 * heads, tokens, HS), BF),
        pltpu.VMEM((tokens, tokens), BF),
        pltpu.VMEM((devices * rows, width), BF),
        pltpu.VMEM((2, line, 2, rows, width), BF),
        pltpu.VMEM((2, line, rows, width), BF),
        pltpu.VMEM((2, line, 2, rows, width), BF),
        pltpu.VMEM((rows, width), F32),
        pltpu.VMEM((2, rows, width), F32),
        pltpu.VMEM((2, rows, HS), F32),
        dma((2, line)), dma((2, line, 2)), dma((2, line)), dma((2, line)),
        dma((2, line, 2)), dma((2, line, 2)),
        dma((2, line, 2)), dma((2, line, 2)), dma((2, line)), dma((2, line)),
        dma((2, line, 2)), dma((2, line, 2)),
        dma((4, heads)), dma((4, heads)), dma((3,)), dma((3,)),
    ]
    return pl.pallas_call(
        layer_kernel,
        in_specs=[pl.BlockSpec(memory_space=pltpu.VMEM)] * 7,
        out_specs=[pl.BlockSpec(memory_space=pltpu.VMEM)] * 6,
        out_shape=[
            shape((tokens, width), BF),
            shape((tokens, width), BF),
            shape((tokens, own), BF),
            shape((tokens, own), BF),
            shape((rows, width), F32),
            shape((rows, width), F32),
        ],
        scratch_shapes=scratch,
        compiler_params=pltpu.CompilerParams(
            collective_id=0, has_side_effects=True, vmem_limit_bytes=67043328
        ),
    )(hidden, queries, attn_keys, w_value, w_out, alpha[None, :], out_grad)


def fits(queries, w_value, alpha, devices):
    rows, own = w_value.shape[0], queries.shape[1]
    unit = 4 * rows
    return (
        devices % 8 == 0
        and rows % 16 == 0
        and unit % HS == 0
        and own * 2 == devices * rows
        and own % unit == 0
        and queries.shape[0] % BLOCK == 0
    )


def sublayer(hidden, queries, attn_keys, w_value, w_out, alpha, out_grad):
    run = layer if fits(queries, w_value, alpha, lax.axis_size("fsdp")) else shards
    return tuple(run(hidden, queries, attn_keys, w_value, w_out, alpha, out_grad))


def solution(mesh):
    placed = (
        P("fsdp", "grp"),
        P("fsdp", "grp"),
        P("fsdp", "grp"),
        P("fsdp", "grp"),
        P("fsdp", "grp"),
        P("grp"),
        P("fsdp", "grp"),
    )
    return jax.shard_map(
        sublayer,
        mesh=mesh,
        in_specs=placed,
        out_specs=(
            P("fsdp", "grp"),
            P("fsdp", "grp"),
            P("fsdp", "grp"),
            P("fsdp", "grp"),
            P("fsdp", "grp"),
            P("fsdp", "grp"),
        ),
        check_vma=False,
    )
```

```python
import jax
import jax.numpy as jnp
from jax import lax
from jax.experimental import pallas as pl
from jax.experimental.pallas import tpu as pltpu
from jax.sharding import PartitionSpec as P

D = 3072
HS = 128


EPS = 1e-06


def contract_last(left, right):
    return lax.dot_general(
        left, right, (((1,), (1,)), ((), ())), preferred_element_type=jnp.float32
    )


def contract_first(left, right):
    return lax.dot_general(
        left, right, (((0,), (0,)), ((), ())), preferred_element_type=jnp.float32
    )


def cost(flops, nbytes):
    return pl.CostEstimate(flops=flops, bytes_accessed=nbytes, transcendentals=0)


def probs_kernel(q_ref, k_ref, probs_ref):
    length = q_ref.shape[0]
    score_scale = q_ref.shape[1] ** (-0.5)
    scores = contract_last(q_ref[...], k_ref[...]) * score_scale
    row_pos = lax.broadcasted_iota(jnp.int32, (length, length), 0)
    col_pos = lax.broadcasted_iota(jnp.int32, (length, length), 1)
    scores = jnp.where(row_pos >= col_pos, scores, -1e30)
    row_peak = jnp.max(scores, axis=1, keepdims=True)
    exp_terms = jnp.exp(scores - row_peak)
    probs_ref[0] = exp_terms * (1.0 / jnp.sum(exp_terms, axis=1, keepdims=True))


def forward_kernel(probs_ref, part_ref, recv_ref, scale_ref, attn_ref, values_ref):
    values = (part_ref[...] + recv_ref[...].astype(jnp.float32)) * scale_ref[...]
    values_b = values.astype(jnp.bfloat16)
    values_ref[...] = values_b
    attn_ref[...] = jnp.dot(
        probs_ref[0].astype(jnp.bfloat16), values_b, preferred_element_type=jnp.float32
    ).astype(jnp.bfloat16)


def backward_kernel(
    probs_ref, q_ref, k_ref, v_ref, part_ref, recv_ref, gq_ref, gk_ref, gv_ref
):
    score_scale = q_ref.shape[1] ** (-0.5)
    grad_head = (part_ref[...] + recv_ref[...].astype(jnp.float32)).astype(jnp.bfloat16)
    probs = probs_ref[0]
    grad_prob = contract_last(grad_head, v_ref[...])
    row_delta = jnp.sum(probs * grad_prob, axis=1, keepdims=True)
    grad_score = (probs * (grad_prob - row_delta)).astype(jnp.bfloat16)
    gv_ref[...] = contract_first(probs.astype(jnp.bfloat16), grad_head).astype(jnp.bfloat16)
    gq_ref[...] = (
        jnp.dot(grad_score, k_ref[...], preferred_element_type=jnp.float32) * score_scale
    ).astype(jnp.bfloat16)
    gk_ref[...] = (contract_first(grad_score, q_ref[...]) * score_scale).astype(jnp.bfloat16)


def head_spec(length):
    return pl.BlockSpec((length, HS), lambda h: (0, h))


def square_spec(length):
    return pl.BlockSpec((1, length, length), lambda h: (h, 0, 0))


def head_probs(queries, keys):
    length, width = queries.shape
    heads = width // HS
    return pl.pallas_call(
        probs_kernel,
        grid=(heads,),
        in_specs=[head_spec(length)] * 2,
        out_specs=square_spec(length),
        out_shape=jax.ShapeDtypeStruct((heads, length, length), jnp.float32),
        cost_estimate=cost(heads * 30 * HS * length * length, 4 * heads * length * length),
    )(queries, keys)


def attend(probs, part, recv, scale):
    length, width = part.shape
    heads = width // HS
    one = head_spec(length)
    shape = jax.ShapeDtypeStruct((length, width), jnp.bfloat16)
    return pl.pallas_call(
        forward_kernel,
        grid=(heads,),
        in_specs=[square_spec(length), one, one, pl.BlockSpec((1, HS), lambda h: (0, h))],
        out_specs=[one, one],
        out_shape=[shape, shape],
        cost_estimate=cost(heads * 4 * HS * length * length, 6 * heads * length * length),
    )(probs, part, recv, scale)


def attend_backward(probs, queries, keys, values, part, recv):
    length, width = part.shape
    heads = width // HS
    one = head_spec(length)
    shape = jax.ShapeDtypeStruct((length, width), jnp.bfloat16)
    return pl.pallas_call(
        backward_kernel,
        grid=(heads,),
        in_specs=[square_spec(length)] + [one] * 5,
        out_specs=[one] * 3,
        out_shape=[shape] * 3,
        cost_estimate=cost(heads * 30 * HS * length * length, 6 * heads * length * length),
    )(probs, queries, keys, values, part, recv)


def shards(hidden, queries, attn_keys, w_value, w_out, alpha, out_grad):
    groups = lax.axis_size("grp")
    assert groups == 2
    me = lax.axis_index("grp")
    swap = [(0, 1), (1, 0)]

    def exchange(block):
        return lax.ppermute(block, "grp", swap)

    def mine_and_other(weight):
        rows = weight.shape[0] // groups
        return (
            lax.dynamic_slice_in_dim(weight, me * rows, rows, 0),
            lax.dynamic_slice_in_dim(weight, (1 - me) * rows, rows, 0),
        )

    def in_order(mine, other):
        return jnp.concatenate(
            (jnp.where(me == 0, mine, other), jnp.where(me == 0, other, mine)), axis=1
        )

    raw_v = lax.all_gather(w_value, "fsdp", axis=0, tiled=True)
    value_rows = w_value.astype(jnp.float32)
    out_rows = w_out.astype(jnp.float32)
    own_sums = jnp.stack(
        (jnp.sum(value_rows * value_rows, axis=1), jnp.sum(out_rows * out_rows, axis=1))
    )
    own_sums = own_sums + exchange(own_sums)
    norms = jnp.sqrt(own_sums + EPS)
    norm_v = norms[0][:, None]
    norm_o = norms[1][:, None]
    unit_v = value_rows / norm_v
    unit_o = out_rows / norm_o
    weight_o = lax.all_gather(unit_o.astype(jnp.bfloat16), "fsdp", axis=0, tiled=True)
    probs = head_probs(queries, attn_keys)

    raw_mine, raw_other = mine_and_other(raw_v)
    value_recv = exchange(contract_last(hidden, raw_other).astype(jnp.bfloat16))
    value_part = contract_last(hidden, raw_mine)
    raw_rows = raw_v.astype(jnp.float32)
    raw_sums = jnp.sum(raw_rows * raw_rows, axis=1)
    all_norm_v = jnp.sqrt(raw_sums + exchange(raw_sums) + EPS)
    width = queries.shape[1]
    scale = 1.0 / lax.dynamic_slice_in_dim(all_norm_v, me * width, width, 0)
    attn_mine, values = attend(probs, value_part, value_recv, scale[None, :])
    weight_v = (raw_v.astype(jnp.float32) / all_norm_v[:, None]).astype(jnp.bfloat16)
    attn_all = in_order(attn_mine, exchange(attn_mine))
    proj = jnp.dot(attn_all, weight_o, preferred_element_type=jnp.float32)
    hidden_f = hidden.astype(jnp.float32)
    keep_rate = 1.0 - alpha
    grad_out = out_grad.astype(jnp.float32)
    moments = jnp.stack(
        (
            jnp.sum(proj * proj, axis=1),
            jnp.sum(keep_rate * keep_rate * hidden_f * hidden_f, axis=1),
            jnp.sum(keep_rate * alpha * hidden_f * proj, axis=1),
            jnp.sum(alpha * alpha * proj * proj, axis=1),
            jnp.sum(grad_out * keep_rate * hidden_f, axis=1),
            jnp.sum(grad_out * alpha * proj, axis=1),
        )
    )
    moments = moments + exchange(moments)
    proj_rs = lax.rsqrt(moments[0] / D + EPS)[:, None]
    cross_sum = moments[2][:, None]
    alpha_sum = moments[3][:, None]
    mix_mean = (moments[1][:, None] + 2.0 * proj_rs * cross_sum + proj_rs * proj_rs * alpha_sum) / D
    mix_rs = lax.rsqrt(mix_mean + EPS)
    mixed = hidden_f + alpha * (proj * proj_rs - hidden_f)
    new_hidden = (mixed * mix_rs).astype(jnp.bfloat16)
    grad_mean = (moments[4][:, None] + proj_rs * moments[5][:, None]) / D
    grad_mix = mix_rs * (grad_out - mixed * mix_rs * mix_rs * grad_mean)
    grad_pn = grad_mix * alpha
    proj_mean = (
        mix_rs * moments[5][:, None]
        - mix_rs * mix_rs * mix_rs * grad_mean * (cross_sum + proj_rs * alpha_sum)
    ) / D
    grad_res = grad_mix * keep_rate
    grad_proj = proj_rs * (grad_pn - proj * proj_rs * proj_rs * proj_mean)
    grad_proj_b = grad_proj.astype(jnp.bfloat16)
    out_mine, out_other = mine_and_other(weight_o)
    grad_recv = exchange(contract_last(grad_proj_b, out_other).astype(jnp.bfloat16))
    grad_part = contract_last(grad_proj_b, out_mine)
    gw_o_own = lax.psum_scatter(
        contract_first(attn_all, grad_proj_b).astype(jnp.bfloat16),
        "fsdp",
        scatter_dimension=0,
        tiled=True,
    ).astype(jnp.float32)
    grad_q, grad_k, grad_v = attend_backward(
        probs, queries, attn_keys, values, grad_part, grad_recv
    )
    grad_values = in_order(grad_v, exchange(grad_v))
    gw_v_own = lax.psum_scatter(
        contract_first(grad_values, hidden).astype(jnp.bfloat16),
        "fsdp",
        scatter_dimension=0,
        tiled=True,
    ).astype(jnp.float32)
    grad_hidden = (
        grad_res + jnp.dot(grad_values, weight_v, preferred_element_type=jnp.float32)
    ).astype(jnp.bfloat16)
    dot_o = jnp.sum(gw_o_own * unit_o, axis=1, keepdims=True)
    dot_o = dot_o + exchange(dot_o)
    grad_w_out = (gw_o_own - unit_o * dot_o) / norm_o
    dot_v = jnp.sum(gw_v_own * unit_v, axis=1, keepdims=True)
    dot_v = dot_v + exchange(dot_v)
    grad_w_value = (gw_v_own - unit_v * dot_v) / norm_v
    return (new_hidden, grad_hidden, grad_q, grad_k, grad_w_value, grad_w_out)


MESH = pl.DeviceIdType.MESH
BLOCK = 256
BF = jnp.bfloat16
F32 = jnp.float32


def nearest(z, s, count):
    reach = jnp.minimum(z, count - 1 - z)
    both = z - (s + 1) // 2 if s % 2 else z + s // 2
    rest = jnp.where(z <= count - 1 - z, s, count - 1 - s)
    return jnp.where(s <= 2 * reach, both, rest)


def layer_kernel(
    wv, wo, alpha, hid_hbm, q_hbm, k_hbm, og_hbm,
    nh_hbm, gh_hbm, gq_hbm, gk_hbm, gwv_hbm, gwo_hbm,
    hid, q, k, og, nh, gh, gq, gk, gwv, gwo, rates2,
    all_v, all_o, probs, nrm, part, xsend, xrecv, vals, attn, proj, gpb, mom, momx, gval,
    grad_s, big_o, ra, rb, rc, acc, fin, dots,
    z_in, z_out, y_in, y_out, c_in, c_out,
    a_in, a_out, b_in, b_out, r_in, r_out, x_in, x_out, s_in, s_out, load_sem, store_sem,
):
    tokens, width = hid.shape
    rows = wv.shape[0]
    heads = part.shape[0]
    devices = all_v.shape[0] // rows
    line = devices // 4
    unit = 4 * rows
    per_unit = unit // HS
    own_units = line // 2
    score_scale = HS ** (-0.5)
    full = 2 * width
    piece = 32 if rows % 32 == 0 else 16
    pieces = rows // piece

    loads = [
        pltpu.make_async_copy(src, dst, load_sem.at[i])
        for i, (src, dst) in enumerate(((q_hbm, q), (k_hbm, k), (hid_hbm, hid), (og_hbm, og)))
    ]
    stores = [
        pltpu.make_async_copy(src, dst, store_sem.at[i])
        for i, (src, dst) in enumerate(
            ((nh, nh_hbm), (gq, gq_hbm), (gk, gk_hbm), (gh, gh_hbm), (gwv, gwv_hbm), (gwo, gwo_hbm))
        )
    ]
    for load in loads:
        load.start()

    me = lax.axis_index("fsdp")
    g = lax.axis_index("grp")
    z = me // 4
    y = lax.rem(me // 2, 2)
    c = lax.rem(me, 2)
    right, left = me + 4, me - 4
    across = z * 4 + (1 - y) * 2 + c
    sibling = z * 4 + y * 2 + (1 - c)
    low = g * own_units
    other_low = (1 - g) * own_units

    def copy(src, dst, out_sem, in_sem, dev):
        return pltpu.make_async_remote_copy(
            src_ref=src, dst_ref=dst, send_sem=out_sem, recv_sem=in_sem,
            device_id=dev, device_id_type=MESH,
        )

    def xcopy(src, dst, kind, h):
        return copy(src, dst, x_out.at[kind, h], x_in.at[kind, h], {"grp": 1 - g})

    def scopy(src, dst, i):
        return copy(src, dst, s_out.at[i], s_in.at[i], {"grp": 1 - g})

    barrier = pltpu.get_barrier_semaphore()

    def greet(dev):
        pl.semaphore_signal(barrier, inc=1, device_id=dev, device_id_type=MESH)

    greet({"grp": 1 - g})
    greet({"fsdp": across})
    greet({"fsdp": sibling})
    pl.when(z > 0)(lambda: greet({"fsdp": left}))
    pl.when(z < line - 1)(lambda: greet({"fsdp": right}))

    lane = lax.broadcasted_iota(jnp.int32, (rows, HS), 1)

    def row_sums(first, second):
        return jnp.where(
            lane == 0,
            jnp.sum(first, axis=1, keepdims=True),
            jnp.sum(second, axis=1, keepdims=True),
        )

    wv_f = wv[...].astype(F32)
    wo_f = wo[...].astype(F32)
    nrm[0] = row_sums(wv_f * wv_f, wo_f * wo_f)
    pl.semaphore_wait(
        barrier, 3 + (z > 0).astype(jnp.int32) + (z < line - 1).astype(jnp.int32)
    )
    norm_copy = scopy(nrm.at[0], nrm.at[1], 0)
    norm_copy.start()

    def cols(h):
        return pl.ds(pl.multiple_of(h * HS, HS), HS)

    def probs_head(h):
        qh = q[:, cols(h)]
        kh = k[:, cols(h)]
        for r in range(tokens // BLOCK):
            top, reach = r * BLOCK, (r + 1) * BLOCK
            scores = contract_last(qh[top:reach], kh[:reach]) * score_scale
            row_pos = lax.broadcasted_iota(jnp.int32, (BLOCK, reach), 0) + top
            col_pos = lax.broadcasted_iota(jnp.int32, (BLOCK, reach), 1)
            scores = jnp.where(row_pos >= col_pos, scores, -1e30)
            terms = jnp.exp(scores - jnp.max(scores, axis=1, keepdims=True))
            total = jnp.sum(terms, axis=1, keepdims=True)
            probs[h, top:reach, :reach] = (terms * (1.0 / total)).astype(BF)

    spread = jnp.broadcast_to(alpha[...][None, :], (16, width))
    rates2[0] = spread
    rates2[1] = 1.0 - spread
    loads[0].wait()
    loads[1].wait()
    probs_head(0)
    norm_copy.wait()
    inv = lax.rsqrt(nrm[0] + nrm[1] + EPS)

    def my_rows(ref):
        return ref.at[pl.ds(pl.multiple_of(me * rows, rows), rows)]

    my_rows(all_v)[...] = (wv[...].astype(F32) * inv[:, 0:1]).astype(BF)
    my_rows(all_o)[...] = (wo[...].astype(F32) * inv[:, 1:2]).astype(BF)

    def shard(ref, u, yy, cc):
        start = pl.multiple_of((u * 4 + yy * 2 + cc) * rows, rows)
        return ref.at[pl.ds(start, rows)]

    def unit_rows(ref, u):
        return ref.at[pl.ds(pl.multiple_of(u * unit, unit), unit)]

    gathered = (all_v, all_o)

    def part_of(ref, p):
        return ref.at[pl.ds(pl.multiple_of(p * piece, piece), piece)]

    def shard_piece(ref, u, yy, cc, p):
        start = pl.multiple_of((u * 4 + yy * 2 + cc) * rows + p * piece, piece)
        return ref.at[pl.ds(start, piece)]

    def each_piece(act):
        lax.fori_loop(0, pieces, lambda p, x: (act(p), x)[1], 0)

    def go_line(w, u, way, dev, p):
        block = shard_piece(gathered[w], u, y, c, p)
        return copy(block, block, z_out.at[w, u, way, p], z_in.at[w, u, p], {"fsdp": dev})

    def go_across(w, u, p):
        block = shard_piece(gathered[w], u, y, c, p)
        return copy(block, block, y_out.at[w, u, p], y_in.at[w, u, p], {"fsdp": across})

    def from_across(w, u, p):
        block = shard_piece(gathered[w], u, 1 - y, c, p)
        return copy(block, block, y_out.at[w, u, p], y_in.at[w, u, p], {"fsdp": across})

    def go_sibling(w, u, yy):
        block = shard(gathered[w], u, yy, c)
        return copy(block, block, c_out.at[w, u, yy], c_in.at[w, u, yy], {"fsdp": sibling})

    def from_sibling(w, u, yy):
        block = shard(gathered[w], u, yy, 1 - c)
        return copy(block, block, c_out.at[w, u, yy], c_in.at[w, u, yy], {"fsdp": sibling})

    def on_line(w, u, p, act):
        pl.when((u <= z) & (z < line - 1))(lambda: act(go_line(w, u, 1, right, p)))
        pl.when((u >= z) & (z > 0))(lambda: act(go_line(w, u, 0, left, p)))

    def gather_piece(w, s, p):
        u = nearest(z, s, line)
        if s:
            go_line(w, u, 0, left, p).wait_recv()
        on_line(w, u, p, lambda d: d.start())
        go_across(w, u, p).start()

    def gather_shard(w, s):
        go_sibling(w, nearest(z, s, line), y).start()

    def gather_step(w, s):
        each_piece(lambda p: gather_piece(w, s, p))
        gather_shard(w, s)

    def gather_across(w, s):
        u = nearest(z, s, line)
        each_piece(lambda p: from_across(w, u, p).wait_recv())
        go_sibling(w, u, 1 - y).start()

    def gather_sibling(w, s):
        u = nearest(z, s, line)
        from_sibling(w, u, 0).wait_recv()
        from_sibling(w, u, 1).wait_recv()

    def gather_drain(w):
        def one(u, carry):
            for p in range(pieces):
                on_line(w, u, p, lambda d: d.wait_send())
                go_across(w, u, p).wait_send()
            go_sibling(w, u, 0).wait_send()
            go_sibling(w, u, 1).wait_send()
            return carry

        lax.fori_loop(0, line, one, 0)

    def is_own(u):
        return (u >= low) & (u < low + own_units)

    def split_heads(kind, u, block):
        @pl.when(is_own(u))
        def _():
            for j in range(per_unit):
                part[(u - low) * per_unit + j] = block[:, j * HS : (j + 1) * HS]

        @pl.when(jnp.logical_not(is_own(u)))
        def _():
            for j in range(per_unit):
                h = (u - other_low) * per_unit + j
                xsend[kind, h] = block[:, j * HS : (j + 1) * HS].astype(BF)
                xcopy(xsend.at[kind, h], xrecv.at[kind, h], 2 * kind, h).start()

    def value_unit(s):
        u = nearest(z, s, line)
        split_heads(0, u, contract_last(hid[...], unit_rows(all_v, u)[...]))

    gather_step(0, 0)
    todo = list(range(1, heads))
    for s in range(1, line):
        while todo and len(todo) > heads - 1 - 2 * s:
            probs_head(todo.pop(0))
        gather_step(0, s)
        if s == line - 1:
            gather_step(1, 0)
        gather_across(0, s - 1)
        gather_sibling(0, s - 1)
        if s == 1:
            loads[2].wait()
        value_unit(s - 1)
    for h in todo:
        probs_head(h)
    gather_across(0, line - 1)
    gather_sibling(0, line - 1)
    value_unit(line - 1)

    def attend_head(h):
        xcopy(xsend.at[0, h], xrecv.at[0, h], 0, h).wait_recv()
        vals[h] = (part[h] + xrecv[0, h].astype(F32)).astype(BF)
        mine = g * heads + h
        for r in range(tokens // BLOCK):
            top, reach = r * BLOCK, (r + 1) * BLOCK
            attn[mine, top:reach] = jnp.dot(
                probs[h, top:reach, :reach], vals[h, :reach], preferred_element_type=F32
            ).astype(BF)
        xcopy(attn.at[mine], attn.at[mine], 1, h).start()

    def own_near(n):
        zc = jnp.clip(z, low, low + own_units - 1) - low
        return nearest(zc, n, own_units)

    def alternate(head, step):
        def both(j, carry):
            head(j)
            step(j)
            return carry

        if pieces == per_unit:
            lax.fori_loop(0, per_unit, both, 0)
        else:
            lax.fori_loop(0, per_unit, lambda j, x: (head(j), x)[1], 0)
            each_piece(step)

    for n in range(own_units):
        u = own_near(n)
        alternate(
            lambda j: attend_head(u * per_unit + j), lambda p: gather_piece(1, 1 + n, p)
        )
        gather_shard(1, 1 + n)
        gather_across(1, n)

    def heads_of(ref, u):
        return jnp.concatenate([ref[u * per_unit + j] for j in range(per_unit)], axis=1)

    def accumulate(ref, u, weight, fresh):
        add = jnp.dot(heads_of(ref, u), unit_rows(weight, u)[...], preferred_element_type=F32)
        if fresh:
            proj[...] = add
        else:
            proj[...] += add

    def project(s):
        u = nearest(z, s, line)
        gather_sibling(1, s)

        @pl.when(jnp.logical_not(is_own(u)))
        def _():
            for j in range(per_unit):
                h = (u - other_low) * per_unit + j
                there = attn.at[(1 - g) * heads + h]
                xcopy(there, there, 1, h).wait_recv()

        accumulate(attn, u, all_o, s == 0)

    for s in range(own_units + 1, line):
        gather_step(1, s)
        gather_across(1, s - 1)
    for s in range(line):
        if s == 1:
            gather_across(1, line - 1)
        project(s)

    step = 16
    inner = 4
    loads[3].wait()

    def chunk(i):
        return pl.ds(pl.multiple_of(i * step, step), step)

    lane16 = lax.broadcasted_iota(jnp.int32, (step, HS), 1)

    def moments(i, carry):
        for n in range(inner):
            r = chunk(i * inner + n)
            rates, keep = rates2[0], rates2[1]
            p = proj[r]
            kh = keep * hid[r].astype(F32)
            ap = rates * p
            go = og[r].astype(F32)
            sums = (p * p, kh * kh, kh * ap, ap * ap, go * kh, go * ap)
            out = jnp.zeros((step, HS), F32)
            for m, term in enumerate(sums):
                out = jnp.where(lane16 == m, jnp.sum(term, axis=1, keepdims=True), out)
            mom[r] = out
        return carry

    lax.fori_loop(0, tokens // (step * inner), moments, 0)
    for i in range(tokens // HS):
        span = slice(i * HS, (i + 1) * HS)
        momx[0, :, span] = jnp.transpose(mom[span])[:8]
    mom_copy = scopy(momx.at[0], momx.at[1], 1)
    mom_copy.start()
    gather_drain(0)
    gather_drain(1)
    mom_copy.wait()
    total = momx[0] + momx[1]
    s_pp, s_hh, s_hp, s_ap, s_gh, s_gp = [total[n : n + 1] for n in range(6)]
    proj_rs = lax.rsqrt(s_pp / full + EPS)
    mix_mean = (s_hh + 2.0 * proj_rs * s_hp + proj_rs * proj_rs * s_ap) / full
    mix_rs = lax.rsqrt(mix_mean + EPS)
    grad_mean = (s_gh + proj_rs * s_gp) / full
    proj_mean = (
        mix_rs * s_gp - mix_rs * mix_rs * mix_rs * grad_mean * (s_hp + proj_rs * s_ap)
    ) / full
    mixed_gain = mix_rs * mix_rs * mix_rs * grad_mean
    proj_gain = proj_rs * proj_rs * proj_rs * proj_mean
    for i in range(tokens // HS):
        span = slice(i * HS, (i + 1) * HS)
        table = [v[:, span] for v in (proj_rs, mix_rs, mixed_gain, proj_gain)]
        table.append(jnp.zeros((HS - len(table), HS), F32))
        mom[span] = jnp.transpose(jnp.concatenate(table, axis=0))

    def mix(i, carry):
        for n in range(inner):
            r = chunk(i * inner + n)
            m = mom[r]
            rates, keep = rates2[0], rates2[1]
            rs, ms, mg, pg = [m[:, j : j + 1] for j in range(4)]
            p = proj[r]
            h = hid[r].astype(F32)
            mixed = h + rates * (p * rs - h)
            nh[r] = (mixed * ms).astype(BF)
            grad_mix = og[r].astype(F32) * ms - mixed * mg
            proj[r] = grad_mix * keep
            gpb[r] = (grad_mix * rates * rs - p * pg).astype(BF)
        return carry

    lax.fori_loop(0, tokens // (step * inner), mix, 0)
    stores[0].start()

    def own_back(n):
        return jnp.where(g == 0, n, line - 1 - n)

    def other_back(n):
        return jnp.where(g == 0, line - 1 - n, n)

    for n in range(own_units):
        u = other_back(n)
        split_heads(1, u, contract_last(gpb[...], unit_rows(all_o, u)[...]))
    for n in range(own_units):
        u = own_back(n)
        split_heads(1, u, contract_last(gpb[...], unit_rows(all_o, u)[...]))

    big = (big_o, all_o)

    def weight_grad(w, ref, other, u):
        add = contract_first(heads_of(ref, u), other[...])
        unit_rows(big[w], u)[...] = add.astype(BF)

    def to_sibling(w, u, yy):
        return copy(
            shard(big[w], u, yy, 1 - c), ra.at[w, u, yy],
            a_out.at[w, u, yy], a_in.at[w, u, yy], {"fsdp": sibling},
        )

    def to_across(w, u, p):
        return copy(
            part_of(ra.at[w, u, 1 - y], p), part_of(rb.at[w, u], p),
            b_out.at[w, u, p], b_in.at[w, u, p], {"fsdp": across},
        )

    def to_line(w, u, way, dev, p):
        return copy(
            part_of(ra.at[w, u, y], p), part_of(rc.at[w, u, 1 - way], p),
            r_out.at[w, u, way, p], r_in.at[w, u, 1 - way, p], {"fsdp": dev},
        )

    def scatter_sibling(w, u):
        to_sibling(w, u, 0).start()
        to_sibling(w, u, 1).start()

    def scatter_across(w, u):
        to_sibling(w, u, 0).wait_recv()
        to_sibling(w, u, 1).wait_recv()

        def one(p):
            mine = part_of(ra.at[w, u, 1 - y], p)
            mine[...] = (
                mine[...].astype(F32)
                + shard_piece(big[w], u, 1 - y, c, p)[...].astype(F32)
            ).astype(BF)
            to_across(w, u, p).start()

        each_piece(one)

    def scatter_piece(w, u, p):
        to_across(w, u, p).wait_recv()
        mine = part_of(ra.at[w, u, y], p)
        acc[...] = (
            shard_piece(big[w], u, y, c, p)[...].astype(F32)
            + mine[...].astype(F32)
            + part_of(rb.at[w, u], p)[...].astype(F32)
        )

        @pl.when((z > 0) & (u >= z))
        def _():
            to_line(w, u, 1, right, p).wait_recv()
            acc[...] += part_of(rc.at[w, u, 0], p)[...].astype(F32)

        @pl.when((z < line - 1) & (u <= z))
        def _():
            to_line(w, u, 0, left, p).wait_recv()
            acc[...] += part_of(rc.at[w, u, 1], p)[...].astype(F32)

        @pl.when(u == z)
        def _():
            part_of(fin.at[w], p)[...] = acc[...]

        @pl.when(u != z)
        def _():
            mine[...] = acc[...].astype(BF)

        pl.when(u > z)(lambda: to_line(w, u, 1, right, p).start())
        pl.when(u < z)(lambda: to_line(w, u, 0, left, p).start())

    def scatter_line(w, u):
        each_piece(lambda p: scatter_piece(w, u, p))

    def scatter_drain(w):
        def one(u, carry):
            to_sibling(w, u, 0).wait_send()
            to_sibling(w, u, 1).wait_send()
            for p in range(pieces):
                to_across(w, u, p).wait_send()
                pl.when(u > z)(lambda: to_line(w, u, 1, right, p).wait_send())
                pl.when(u < z)(lambda: to_line(w, u, 0, left, p).wait_send())
            return carry

        lax.fori_loop(0, line, one, 0)

    far_first = [line - 1 - s for s in range(line)]
    for n, s in enumerate(far_first):
        u = nearest(z, s, line)
        weight_grad(0, attn, gpb, u)
        scatter_sibling(0, u)
        if n:
            scatter_across(0, nearest(z, far_first[n - 1], line))
    scatter_across(0, nearest(z, 0, line))

    def back_head(h):
        xcopy(xsend.at[1, h], xrecv.at[1, h], 2, h).wait_recv()
        mine = g * heads + h
        grad_head = (part[h] + xrecv[1, h].astype(F32)).astype(BF)
        qh = q[:, cols(h)]
        kh = k[:, cols(h)]
        vh = vals[h]
        for r in range(tokens // BLOCK):
            top, reach = r * BLOCK, (r + 1) * BLOCK
            p = probs[h, top:reach, :reach].astype(F32)
            grad_prob = contract_last(grad_head[top:reach], vh[:reach])
            delta = jnp.sum(p * grad_prob, axis=1, keepdims=True)
            grad_score = (p * (grad_prob - delta)).astype(BF)
            grad_s[top:reach, :reach] = grad_score
            gq[top:reach, cols(h)] = (
                jnp.dot(grad_score, kh[:reach], preferred_element_type=F32) * score_scale
            ).astype(BF)
        for r in range(tokens // BLOCK):
            top, reach = r * BLOCK, (r + 1) * BLOCK
            gval[mine, top:reach] = contract_first(
                probs[h, top:, top:reach], grad_head[top:]
            ).astype(BF)
            gk[top:reach, cols(h)] = (
                contract_first(grad_s[top:, top:reach], qh[top:]) * score_scale
            ).astype(BF)
        xcopy(gval.at[mine], gval.at[mine], 3, h).start()

    for n in range(own_units):
        u = own_back(n)
        far = nearest(z, far_first[n], line)
        alternate(
            lambda j: back_head((u - low) * per_unit + j), lambda p: scatter_piece(0, far, p)
        )
        weight_grad(1, gval, hid, u)
        scatter_sibling(1, u)
        scatter_across(1, u)
    stores[1].start()
    stores[2].start()
    for n in range(own_units):
        accumulate(gval, own_back(n), all_v, False)
        scatter_line(0, nearest(z, far_first[own_units + n], line))

    for n in range(own_units):
        u = other_back(n)
        for j in range(per_unit):
            h = (u - other_low) * per_unit + j
            there = gval.at[(1 - g) * heads + h]
            xcopy(there, there, 3, h).wait_recv()
        weight_grad(1, gval, hid, u)
        scatter_sibling(1, u)
        scatter_across(1, u)
        accumulate(gval, u, all_v, False)
    gh[...] = proj[...].astype(BF)
    stores[3].start()

    inv = lax.rsqrt(nrm[0] + nrm[1] + EPS)
    unit_v = wv[...].astype(F32) * inv[:, 0:1]
    unit_o = wo[...].astype(F32) * inv[:, 1:2]
    here = jnp.where((z < own_units) == (g == 0), 0, own_units) + jnp.minimum(z, line - 1 - z)

    def line_step(n, carry):
        m = n + (n >= here).astype(jnp.int32)
        first = jnp.where(m < own_units, m, m - own_units)
        from_low = (m < own_units) == (g == 0)
        u = jnp.where(from_low, first, line - 1 - first)
        scatter_line(1, jnp.where(n == line - 1, z, u))
        return carry

    lax.fori_loop(0, line, line_step, 0)
    dots[0] = row_sums(fin[1] * unit_v, fin[0] * unit_o)
    dot_copy = scopy(dots.at[0], dots.at[1], 2)
    dot_copy.start()
    scatter_drain(0)
    scatter_drain(1)

    def drain(h, carry):
        xcopy(xsend.at[0, h], xrecv.at[0, h], 0, h).wait_send()
        xcopy(xsend.at[1, h], xrecv.at[1, h], 2, h).wait_send()
        mine = g * heads + h
        xcopy(attn.at[mine], attn.at[mine], 1, h).wait_send()
        xcopy(gval.at[mine], gval.at[mine], 3, h).wait_send()
        return carry

    lax.fori_loop(0, heads, drain, 0)
    dot_copy.wait()
    total = dots[0] + dots[1]
    gwv[...] = (fin[1] - unit_v * total[:, 0:1]) * inv[:, 0:1]
    gwo[...] = (fin[0] - unit_o * total[:, 1:2]) * inv[:, 1:2]
    stores[4].start()
    stores[5].start()
    for store in stores:
        store.wait()


def move_kernel(*refs):
    count = (len(refs) - 1) // 3
    ins, outs, held = refs[:count], refs[count : 2 * count], refs[2 * count : 3 * count]
    sems = refs[3 * count]
    reads, writes = [], []
    for i in range(count):
        half = held[i].shape[0] // 2
        for j in range(2):
            part = pl.ds(j * half, half)
            reads.append(
                pltpu.make_async_copy(ins[i].at[part], held[i].at[part], sems.at[0, i, j])
            )
            writes.append(
                pltpu.make_async_copy(held[i].at[part], outs[i].at[part], sems.at[1, i, j])
            )
    for read in reads:
        read.start()
    for read, write in zip(reads, writes):
        read.wait()
        write.start()
    for write in writes:
        write.wait()


def move_out(arrays):
    anywhere = pl.BlockSpec(memory_space=pl.ANY)
    return pl.pallas_call(
        move_kernel,
        in_specs=[anywhere] * len(arrays),
        out_specs=[anywhere] * len(arrays),
        out_shape=[jax.ShapeDtypeStruct(a.shape, a.dtype) for a in arrays],
        scratch_shapes=[pltpu.VMEM(a.shape, a.dtype) for a in arrays]
        + [pltpu.SemaphoreType.DMA((2, len(arrays), 2))],
    )(*arrays)


def layer(hidden, queries, attn_keys, w_value, w_out, alpha, out_grad):
    tokens, width = hidden.shape
    rows = w_value.shape[0]
    own = queries.shape[1]
    heads = own // HS
    devices = lax.axis_size("fsdp")
    line = devices // 4
    head_block = (heads, tokens, HS)
    dma = pltpu.SemaphoreType.DMA
    shape = jax.ShapeDtypeStruct
    piece = 32 if rows % 32 == 0 else 16
    pieces = rows // piece
    scratch = [
        pltpu.VMEM((tokens, width), BF),
        pltpu.VMEM((tokens, own), BF),
        pltpu.VMEM((tokens, own), BF),
        pltpu.VMEM((tokens, width), BF),
        pltpu.VMEM((tokens, width), BF),
        pltpu.VMEM((tokens, width), BF),
        pltpu.VMEM((tokens, own), BF),
        pltpu.VMEM((tokens, own), BF),
        pltpu.VMEM((rows, width), F32),
        pltpu.VMEM((rows, width), F32),
        pltpu.VMEM((2, 16, width), F32),
        pltpu.VMEM((devices * rows, width), BF),
        pltpu.VMEM((devices * rows, width), BF),
        pltpu.VMEM((heads, tokens, tokens), BF),
        pltpu.VMEM((2, rows, HS), F32),
        pltpu.VMEM(head_block, F32),
        pltpu.VMEM((2,) + head_block, BF),
        pltpu.VMEM((2,) + head_block, BF),
        pltpu.VMEM(head_block, BF),
        pltpu.VMEM((2 * heads, tokens, HS), BF),
        pltpu.VMEM((tokens, width), F32),
        pltpu.VMEM((tokens, width), BF),
        pltpu.VMEM((tokens, HS), F32),
        pltpu.VMEM((2, 8, tokens), F32),
        pltpu.VMEM((2 * heads, tokens, HS), BF),
        pltpu.VMEM((tokens, tokens), BF),
        pltpu.VMEM((devices * rows, width), BF),
        pltpu.VMEM((2, line, 2, rows, width), BF),
        pltpu.VMEM((2, line, rows, width), BF),
        pltpu.VMEM((2, line, 2, rows, width), BF),
        pltpu.VMEM((piece, width), F32),
        pltpu.VMEM((2, rows, width), F32),
        pltpu.VMEM((2, rows, HS), F32),
        dma((2, line, pieces)), dma((2, line, 2, pieces)),
        dma((2, line, pieces)), dma((2, line, pieces)),
        dma((2, line, 2)), dma((2, line, 2)),
        dma((2, line, 2)), dma((2, line, 2)),
        dma((2, line, pieces)), dma((2, line, pieces)),
        dma((2, line, 2, pieces)), dma((2, line, 2, pieces)),
        dma((4, heads)), dma((4, heads)), dma((3,)), dma((3,)), dma((4,)), dma((6,)),
    ]
    anywhere = pl.BlockSpec(memory_space=pl.ANY)
    outs = pl.pallas_call(
        layer_kernel,
        in_specs=[pl.BlockSpec(memory_space=pltpu.VMEM)] * 3 + [anywhere] * 4,
        out_specs=[anywhere] * 6,
        out_shape=[
            shape((tokens, width), BF),
            shape((tokens, width), BF),
            shape((tokens, own), BF),
            shape((tokens, own), BF),
            shape((rows, width), F32),
            shape((rows, width), F32),
        ],
        scratch_shapes=scratch,
        compiler_params=pltpu.CompilerParams(
            collective_id=0, has_side_effects=True, vmem_limit_bytes=67043328
        ),
    )(w_value, w_out, alpha, hidden, queries, attn_keys, out_grad)
    return move_out(outs)


def fits(queries, w_value, alpha, devices):
    rows, own = w_value.shape[0], queries.shape[1]
    unit = 4 * rows
    return (
        devices % 8 == 0
        and rows % 16 == 0
        and unit % HS == 0
        and own * 2 == devices * rows
        and own % unit == 0
        and queries.shape[0] % BLOCK == 0
    )


def sublayer(hidden, queries, attn_keys, w_value, w_out, alpha, out_grad):
    run = layer if fits(queries, w_value, alpha, lax.axis_size("fsdp")) else shards
    return tuple(run(hidden, queries, attn_keys, w_value, w_out, alpha, out_grad))


def solution(mesh):
    placed = (
        P("fsdp", "grp"),
        P("fsdp", "grp"),
        P("fsdp", "grp"),
        P("fsdp", "grp"),
        P("fsdp", "grp"),
        P("grp"),
        P("fsdp", "grp"),
    )
    return jax.shard_map(
        sublayer,
        mesh=mesh,
        in_specs=placed,
        out_specs=(
            P("fsdp", "grp"),
            P("fsdp", "grp"),
            P("fsdp", "grp"),
            P("fsdp", "grp"),
            P("fsdp", "grp"),
            P("fsdp", "grp"),
        ),
        check_vma=False,
    )
```
